32 devices in a mesh: gx: 2 (over y), gy: 4 (over x, core), gz: 4 (over z).
Axes of the slice: x: 2, y: 2, z: 4, core: 2. Of those that a mesh axis runs over, the one named last changes fastest.
Arguments:
- head_out: bfloat16 [768, 4096], P(('gy', 'gx'), 'gz'), may hold values from -6 to 6
- out_weight: bfloat16 [4096, 4096], P('gz', ('gx', 'gy')), may hold values from -0.09375 to 0.09375
- residual: bfloat16 [768, 4096], P(('gy', 'gz'), 'gx'), may hold values from -84 to 84
- norm_gain: bfloat16 [4096], replicated, may hold values from 0.5 to 1.5
Outputs:
- hidden_out: bfloat16 [768, 4096], P(('gy', 'gz'), 'gx')
- normed: bfloat16 [768, 4096], P(('gy', 'gz'), 'gx')
The draws below stay inside these ranges and needn't reach their ends.
All inputs are finite; a program needn't handle non-finite values.
Results may differ from the reference program's by a relative error of at most 0.0098.
Values may be sent and summed in bfloat16 or wider, within the bound.
A program may use at most 64 MiB of HBM per device.

```python
import math
import jax
import jax.numpy as jnp
from jax import lax

D = 4096
FEATURES = 4096
TOKENS = 768


def draw_residual(key, part):
    key_base, key_rows, key_cols = jax.random.split(jax.random.fold_in(key, 11), 3)
    col_pos = jnp.arange(D, dtype=jnp.float32) / D
    col_ramp = jnp.exp((col_pos - 0.5) * math.log(3.0))
    col_spread = jnp.exp(jax.random.uniform(key_cols, (1, D), jnp.float32, math.log(0.5), math.log(2.0)))
    base_draw = jnp.clip(jax.random.normal(key_base, (TOKENS, D), jnp.float32), -6.0, 6.0)
    row_scale = jnp.exp(jax.random.uniform(key_rows, (TOKENS, 1), jnp.float32, math.log(0.4), math.log(4.0)))
    return (base_draw * row_scale * col_spread * col_ramp[None, :]).astype(jnp.bfloat16)


def with_spikes(result, key, source, target, parts, factor):
    owner, partner = [(jnp.arange(result.shape[axis_at]) // (result.shape[axis_at] // parts)).reshape([-1 if axis == axis_at else 1 for axis in range(result.ndim)]) for axis_at in (source, target)]
    chosen = jax.random.permutation(key, parts)[partner]
    strong = (owner == chosen) | (owner == (partner + parts // 2) % parts)
    return jnp.where(strong, factor * result, result)


def level_of(stream_key, extent, cuts, least, largest):
    gain = 1.0
    for position, parts in cuts:
        heights = jax.random.uniform(jax.random.fold_in(jax.random.fold_in(stream_key, 6), position), (parts,), jnp.float32, least / len(cuts), largest / len(cuts))
        gain = gain * jnp.repeat(jnp.exp(heights), extent[position] // parts).reshape((-1,) + (1,) * (len(extent) - 1 - position))
    return gain


def gaussian(key, extent, deviation, bound, shards=(), kind=jnp.bfloat16):
    values = deviation * jax.random.normal(key, extent, jnp.float32)
    if shards:
        values = values * level_of(key, extent, shards, -0.22, 0.18)
    return jnp.clip(values, -bound, bound).astype(kind)


def noise_with(own_key, shape, spread, most, shards, heavy, held_as=jnp.bfloat16):
    entries = spread * jax.random.normal(own_key, shape, jnp.float32)
    if shards:
        entries = entries * level_of(own_key, shape, shards, -0.22, 0.18)
    return jnp.clip(with_spikes(entries, jax.random.fold_in(own_key, 3), *heavy), -most, most).astype(held_as)


def setup_inputs(seed: int = 0) -> dict:
    key_list = jax.random.split(jax.random.key(seed), 5)
    head_out = noise_with(key_list[0], (TOKENS, FEATURES), 1.0, 6.0, ((0, 8), (1, 4)), (1, 0, 8, 2.0))
    out_weight = gaussian(key_list[1], (FEATURES, D), FEATURES ** -0.5, 0.09375, ((0, 4), (1, 8)))
    residual = draw_residual(jax.random.fold_in(key_list[4], 71), 0)
    norm_gain = jnp.clip(1.0 + 0.1 * jax.random.normal(key_list[3], (D,), jnp.float32), 0.5, 1.5).astype(jnp.bfloat16)
    return dict(head_out=head_out, out_weight=out_weight, residual=residual, norm_gain=norm_gain)


def reference(head_out, out_weight, residual, norm_gain):
    projected = jnp.dot(head_out, out_weight, preferred_element_type=jnp.float32)
    hidden = (residual.astype(jnp.float32) + projected).astype(jnp.bfloat16)
    widened = lax.optimization_barrier(hidden).astype(jnp.float32)
    inverse = lax.rsqrt(lax.optimization_barrier(jnp.mean(widened * widened, axis=1, keepdims=True)) + 1e-05)
    normed = (widened * inverse * norm_gain.astype(jnp.float32)).astype(jnp.bfloat16)
    return (hidden, normed)
```

```python
import functools

import jax
import jax.numpy as jnp
from jax import lax
from jax.experimental import pallas as pl
from jax.experimental.pallas import tpu as pltpu
from jax.sharding import PartitionSpec as P

MESH = pl.DeviceIdType.MESH
F32 = jnp.float32
BF16 = jnp.bfloat16
CORES = 2


def kernel(ny, ngy, nz, head_ref, w_ref, res_ref, gain_ref, hid_ref, nrm_ref,
           heads, w_own, w_other, res_v, send_buf, recv, own, sums,
           local_sem, w_send, w_recv, h_send, h_recv, p_send, p_recv, s_send, s_recv):
    nx = ngy // CORES
    y = lax.axis_index("gx")
    gy = lax.axis_index("gy")
    z = lax.axis_index("gz")
    x, core = lax.div(gy, CORES), lax.rem(gy, CORES)
    in_rows = head_ref.shape[0]
    out_rows, cols = res_ref.shape
    wc = w_ref.shape[1]
    per_block = nz // ny

    def at(dx, dy, dz):
        return (lax.rem(y + dy + ny, ny), lax.rem(x + dx + nx, nx) * CORES + core, lax.rem(z + dz + nz, nz))

    partner = (y, x * CORES + 1 - core, z)
    offsets = {(dx, dy, 0) for dx in range(nx) for dy in range(ny)} | {(dx, 0, dz) for dx in range(nx) for dz in range(nz)}
    offsets = sorted(offsets - {(0, 0, 0)})
    barrier = pltpu.get_barrier_semaphore()
    pl.semaphore_signal(barrier, inc=1, device_id=partner, device_id_type=MESH)
    for off in offsets:
        pl.semaphore_signal(barrier, inc=1, device_id=at(*off), device_id_type=MESH)

    head_in = pltpu.make_async_copy(head_ref, heads.at[0, 0], local_sem.at[0])
    w_in = pltpu.make_async_copy(w_ref, w_own, local_sem.at[1])
    res_in = pltpu.make_async_copy(res_ref, res_v, local_sem.at[2])
    head_in.start()
    w_in.start()
    res_in.start()
    head_in.wait()
    pl.semaphore_wait(barrier, len(offsets) + 1)

    blocks = sorted(((dx, dy) for dx in range(nx) for dy in range(ny)), key=lambda b: ((b[0] > 0) + (b[1] > 0), b))
    head_copies = {}
    for dx, dy in blocks[1:]:
        head_copies[dx, dy] = pltpu.make_async_remote_copy(
            src_ref=heads.at[0, 0], dst_ref=heads.at[dx, dy],
            send_sem=h_send.at[dx, dy], recv_sem=h_recv.at[dx, dy],
            device_id=at(-dx, -dy, 0), device_id_type=MESH)
        head_copies[dx, dy].start()
    w_in.wait()
    w_copy = pltpu.make_async_remote_copy(
        src_ref=w_own, dst_ref=w_other, send_sem=w_send, recv_sem=w_recv,
        device_id=partner, device_id_type=MESH)
    w_copy.start()

    def chunk(dx, dy, hr, j):
        to_z = lax.rem(y + dy, ny) * per_block + j
        dz = lax.rem(to_z - z + nz, nz)
        copy = pltpu.make_async_remote_copy(
            src_ref=send_buf.at[dx, dy, hr, pl.ds(j * out_rows, out_rows)],
            dst_ref=recv.at[dx, dz, hr],
            send_sem=p_send.at[dx, dy, hr, j], recv_sem=p_recv.at[dx, dz, hr],
            device_id=(y, lax.rem(x + dx, nx) * CORES + core, to_z), device_id_type=MESH)
        return to_z, copy

    for dx, dy in blocks:
        if (dx, dy) != (0, 0):
            head_copies[dx, dy].wait_recv()
        for hr in range(CORES):
            if (dx, dy) == (0, 0) and hr == 1:
                w_copy.wait_recv()
            part = jnp.dot(heads[dx, dy], (w_other if hr else w_own)[...], preferred_element_type=F32)
            send_buf[dx, dy, hr] = part.astype(BF16)
            for j in range(per_block):
                to_z, copy = chunk(dx, dy, hr, j)
                if dx:
                    copy.start()
                else:
                    pl.when(to_z != z)(copy.start)

                    @pl.when(to_z == z)
                    def _():
                        own[hr] = part[j * out_rows:(j + 1) * out_rows]

    res_in.wait()
    total = jnp.zeros((out_rows, 128), F32)
    for dx in range(nx):
        from_x = lax.rem(x - dx + nx, nx)
        for hr in range(CORES):
            half = core if hr == 0 else 1 - core
            where = pl.ds(pl.multiple_of((from_x * CORES + half) * wc, wc), wc)
            acc = own[hr] if dx == 0 else None
            for dz in range(nz):
                if (dx, dz) == (0, 0):
                    continue
                pltpu.make_async_remote_copy(
                    src_ref=send_buf.at[0, 0, hr, pl.ds(0, out_rows)], dst_ref=recv.at[dx, dz, hr],
                    send_sem=p_send.at[0, 0, hr, 0], recv_sem=p_recv.at[dx, dz, hr],
                    device_id=partner, device_id_type=MESH).wait_recv()
                term = recv[dx, dz, hr].astype(F32)
                acc = term if acc is None else acc + term
            hidden = (res_v[:, where].astype(F32) + acc).astype(BF16)
            hid_ref[:, where] = hidden
            wide = hidden.astype(F32)
            square = wide * wide
            for k in range(0, wc, 128):
                total = total + square[:, k:k + 128]
    sums[0] = jnp.broadcast_to(jnp.sum(total, axis=1, keepdims=True), (out_rows, 128))
    sum_copies = []
    for dy in range(1, ny):
        sum_copies.append(pltpu.make_async_remote_copy(
            src_ref=sums.at[0], dst_ref=sums.at[dy], send_sem=s_send.at[dy], recv_sem=s_recv.at[dy],
            device_id=at(0, -dy, 0), device_id_type=MESH))
        sum_copies[-1].start()

    w_copy.wait_send()
    for copy in head_copies.values():
        copy.wait_send()
    for dx, dy in blocks:
        for hr in range(CORES):
            for j in range(per_block):
                to_z, copy = chunk(dx, dy, hr, j)
                if dx:
                    copy.wait_send()
                else:
                    pl.when(to_z != z)(copy.wait_send)
    squares = sums[0]
    for dy, copy in enumerate(sum_copies, 1):
        copy.wait()
        squares = squares + sums[dy]
    inverse = lax.rsqrt(squares / (cols * ny) + 1e-05)[:, :1]
    gain = gain_ref[:, pl.ds(pl.multiple_of(y * cols, cols), cols)]
    nrm_ref[...] = (hid_ref[...].astype(F32) * inverse * gain).astype(BF16)


def shards(head_out, out_weight, residual, norm_gain):
    ny, ngy, nz = (lax.axis_size(a) for a in ("gx", "gy", "gz"))
    nx = ngy // CORES
    in_rows, depth = head_out.shape
    wc = out_weight.shape[1]
    out_rows, cols = residual.shape
    per_block = nz // ny
    any_spec = pl.BlockSpec(memory_space=pl.ANY)
    vmem = pl.BlockSpec(memory_space=pltpu.VMEM)
    dma = pltpu.SemaphoreType.DMA
    return pl.pallas_call(
        functools.partial(kernel, ny, ngy, nz),
        out_shape=[jax.ShapeDtypeStruct((out_rows, cols), BF16)] * 2,
        in_specs=[any_spec, any_spec, any_spec, vmem],
        out_specs=[vmem, vmem],
        scratch_shapes=[
            pltpu.VMEM((nx, ny, in_rows, depth), BF16),
            pltpu.VMEM((depth, wc), BF16),
            pltpu.VMEM((depth, wc), BF16),
            pltpu.VMEM((out_rows, cols), BF16),
            pltpu.VMEM((nx, ny, CORES, in_rows, wc), BF16),
            pltpu.VMEM((nx, nz, CORES, out_rows, wc), BF16),
            pltpu.VMEM((CORES, out_rows, wc), F32),
            pltpu.VMEM((ny, out_rows, 128), F32),
            dma((3,)), dma, dma, dma((nx, ny)), dma((nx, ny)),
            dma((nx, ny, CORES, per_block)), dma((nx, nz, CORES)),
            dma((ny,)), dma((ny,)),
        ],
        compiler_params=pltpu.CompilerParams(collective_id=0, has_side_effects=True),
    )(head_out, out_weight, residual, norm_gain.astype(F32).reshape(1, -1))


def solution(mesh):
    in_specs = (P(("gy", "gx"), "gz"), P("gz", ("gx", "gy")), P(("gy", "gz"), "gx"), P())
    out_specs = (P(("gy", "gz"), "gx"), P(("gy", "gz"), "gx"))
    return jax.shard_map(shards, mesh=mesh, in_specs=in_specs, out_specs=out_specs, check_vma=False)
```

```python
import functools

import jax
import jax.numpy as jnp
from jax import lax
from jax.experimental import pallas as pl
from jax.experimental.pallas import tpu as pltpu
from jax.sharding import PartitionSpec as P

MESH = pl.DeviceIdType.MESH
F32 = jnp.float32
BF16 = jnp.bfloat16
CORES = 2


def kernel(ny, ngy, nz, head_ref, w_ref, res_ref, gain_ref, hid_ref, nrm_ref,
           heads, w_own, w_other, res_v, send_buf, recv, own, back, sums,
           local_sem, w_send, w_recv, h_send, h_recv, p_send, p_recv, b_send, b_recv, s_send, s_recv):
    nx = ngy // CORES
    y = lax.axis_index("gx")
    gy = lax.axis_index("gy")
    z = lax.axis_index("gz")
    x, core = lax.div(gy, CORES), lax.rem(gy, CORES)
    in_rows = head_ref.shape[0]
    out_rows, cols = res_ref.shape
    wc = w_ref.shape[1]
    per_block = nz // ny

    def at(dx, dy, dz):
        return (lax.rem(y + dy + ny, ny), lax.rem(x + dx + nx, nx) * CORES + core, lax.rem(z + dz + nz, nz))

    partner = (y, x * CORES + 1 - core, z)
    offsets = {(dx, dy, 0) for dx in range(nx) for dy in range(ny)} | {(0, 0, dz) for dz in range(nz)}
    offsets = sorted(offsets - {(0, 0, 0)})
    barrier = pltpu.get_barrier_semaphore()
    pl.semaphore_signal(barrier, inc=1, device_id=partner, device_id_type=MESH)
    for off in offsets:
        pl.semaphore_signal(barrier, inc=1, device_id=at(*off), device_id_type=MESH)

    head_in = pltpu.make_async_copy(head_ref, heads.at[0, 0], local_sem.at[0])
    w_in = pltpu.make_async_copy(w_ref, w_own, local_sem.at[1])
    res_in = pltpu.make_async_copy(res_ref, res_v, local_sem.at[2])
    head_in.start()
    w_in.start()
    res_in.start()
    head_in.wait()
    pl.semaphore_wait(barrier, len(offsets) + 1)

    blocks = sorted(((dx, dy) for dx in range(nx) for dy in range(ny)), key=lambda b: ((b[0] > 0) + (b[1] > 0), -b[0], b))
    head_copies = {}
    for dx, dy in blocks[1:]:
        head_copies[dx, dy] = pltpu.make_async_remote_copy(
            src_ref=heads.at[0, 0], dst_ref=heads.at[dx, dy],
            send_sem=h_send.at[dx, dy], recv_sem=h_recv.at[dx, dy],
            device_id=at(-dx, -dy, 0), device_id_type=MESH)
        head_copies[dx, dy].start()
    w_in.wait()
    w_copy = pltpu.make_async_remote_copy(
        src_ref=w_own, dst_ref=w_other, send_sem=w_send, recv_sem=w_recv,
        device_id=partner, device_id_type=MESH)
    w_copy.start()

    def chunk(dx, dy, hr, j):
        to_z = lax.rem(y + dy, ny) * per_block + j
        dz = lax.rem(to_z - z + nz, nz)
        copy = pltpu.make_async_remote_copy(
            src_ref=send_buf.at[dx, dy, hr, pl.ds(j * out_rows, out_rows)],
            dst_ref=recv.at[dx, dz, hr],
            send_sem=p_send.at[dx, dy, hr, j], recv_sem=p_recv.at[dx, dz, hr],
            device_id=(y, gy, to_z), device_id_type=MESH)
        return to_z, copy

    for dx, dy in blocks:
        if (dx, dy) != (0, 0):
            head_copies[dx, dy].wait_recv()
        for hr in range(CORES):
            if (dx, dy) == (0, 0) and hr == 1:
                w_copy.wait_recv()
            part = jnp.dot(heads[dx, dy], (w_other if hr else w_own)[...], preferred_element_type=F32)
            send_buf[dx, dy, hr] = part.astype(BF16)
            for j in range(per_block):
                to_z, copy = chunk(dx, dy, hr, j)
                pl.when(to_z != z)(copy.start)

                @pl.when(to_z == z)
                def _():
                    own[dx, hr] = part[j * out_rows:(j + 1) * out_rows]

    def reduced(dx, hr):
        acc = own[dx, hr]
        for dz in range(1, nz):
            pltpu.make_async_remote_copy(
                src_ref=send_buf.at[0, 0, hr, pl.ds(0, out_rows)], dst_ref=recv.at[dx, dz, hr],
                send_sem=p_send.at[0, 0, hr, 0], recv_sem=p_recv.at[dx, dz, hr],
                device_id=partner, device_id_type=MESH).wait_recv()
            acc = acc + recv[dx, dz, hr].astype(F32)
        return acc

    back_copies = {}
    for dx in range(1, nx):
        for hr in range(CORES):
            back[0, dx, hr] = reduced(dx, hr).astype(BF16)
            back_copies[dx, hr] = pltpu.make_async_remote_copy(
                src_ref=back.at[0, dx, hr], dst_ref=back.at[1, dx, hr],
                send_sem=b_send.at[dx, hr], recv_sem=b_recv.at[dx, hr],
                device_id=at(dx, 0, 0), device_id_type=MESH)
            back_copies[dx, hr].start()

    res_in.wait()
    total = jnp.zeros((out_rows, 128), F32)
    for dx in range(nx):
        from_x = lax.rem(x - dx + nx, nx)
        for hr in range(CORES):
            half = core if hr == 0 else 1 - core
            where = pl.ds(pl.multiple_of((from_x * CORES + half) * wc, wc), wc)
            if dx:
                back_copies[dx, hr].wait_recv()
                acc = back[1, dx, hr].astype(F32)
            else:
                acc = reduced(0, hr)
            hidden = (res_v[:, where].astype(F32) + acc).astype(BF16)
            hid_ref[:, where] = hidden
            wide = hidden.astype(F32)
            square = wide * wide
            for k in range(0, wc, 128):
                total = total + square[:, k:k + 128]
    sums[0] = jnp.broadcast_to(jnp.sum(total, axis=1, keepdims=True), (out_rows, 128))
    sum_copies = []
    for dy in range(1, ny):
        sum_copies.append(pltpu.make_async_remote_copy(
            src_ref=sums.at[0], dst_ref=sums.at[dy], send_sem=s_send.at[dy], recv_sem=s_recv.at[dy],
            device_id=at(0, -dy, 0), device_id_type=MESH))
        sum_copies[-1].start()

    w_copy.wait_send()
    for copy in list(head_copies.values()) + list(back_copies.values()):
        copy.wait_send()
    for dx, dy in blocks:
        for hr in range(CORES):
            for j in range(per_block):
                to_z, copy = chunk(dx, dy, hr, j)
                pl.when(to_z != z)(copy.wait_send)
    squares = sums[0]
    for dy, copy in enumerate(sum_copies, 1):
        copy.wait()
        squares = squares + sums[dy]
    inverse = lax.rsqrt(squares / (cols * ny) + 1e-05)[:, :1]
    gain = gain_ref[:, pl.ds(pl.multiple_of(y * cols, cols), cols)]
    nrm_ref[...] = (hid_ref[...].astype(F32) * inverse * gain).astype(BF16)


def shards(head_out, out_weight, residual, norm_gain):
    ny, ngy, nz = (lax.axis_size(a) for a in ("gx", "gy", "gz"))
    nx = ngy // CORES
    in_rows, depth = head_out.shape
    wc = out_weight.shape[1]
    out_rows, cols = residual.shape
    per_block = nz // ny
    any_spec = pl.BlockSpec(memory_space=pl.ANY)
    vmem = pl.BlockSpec(memory_space=pltpu.VMEM)
    dma = pltpu.SemaphoreType.DMA
    return pl.pallas_call(
        functools.partial(kernel, ny, ngy, nz),
        out_shape=[jax.ShapeDtypeStruct((out_rows, cols), BF16)] * 2,
        in_specs=[any_spec, any_spec, any_spec, vmem],
        out_specs=[vmem, vmem],
        scratch_shapes=[
            pltpu.VMEM((nx, ny, in_rows, depth), BF16),
            pltpu.VMEM((depth, wc), BF16),
            pltpu.VMEM((depth, wc), BF16),
            pltpu.VMEM((out_rows, cols), BF16),
            pltpu.VMEM((nx, ny, CORES, in_rows, wc), BF16),
            pltpu.VMEM((nx, nz, CORES, out_rows, wc), BF16),
            pltpu.VMEM((nx, CORES, out_rows, wc), F32),
            pltpu.VMEM((2, nx, CORES, out_rows, wc), BF16),
            pltpu.VMEM((ny, out_rows, 128), F32),
            dma((3,)), dma, dma, dma((nx, ny)), dma((nx, ny)),
            dma((nx, ny, CORES, per_block)), dma((nx, nz, CORES)),
            dma((nx, CORES)), dma((nx, CORES)),
            dma((ny,)), dma((ny,)),
        ],
        compiler_params=pltpu.CompilerParams(collective_id=0, has_side_effects=True),
    )(head_out, out_weight, residual, norm_gain.astype(F32).reshape(1, -1))


def solution(mesh):
    in_specs = (P(("gy", "gx"), "gz"), P("gz", ("gx", "gy")), P(("gy", "gz"), "gx"), P())
    out_specs = (P(("gy", "gz"), "gx"), P(("gy", "gz"), "gx"))
    return jax.shard_map(shards, mesh=mesh, in_specs=in_specs, out_specs=out_specs, check_vma=False)
```

```python
import functools

import jax
import jax.numpy as jnp
from jax import lax
from jax.experimental import pallas as pl
from jax.experimental.pallas import tpu as pltpu
from jax.sharding import PartitionSpec as P

MESH = pl.DeviceIdType.MESH
F32 = jnp.float32
BF16 = jnp.bfloat16
CORES = 2


def kernel(ny, ngy, nz, head_ref, w_ref, res_ref, gain_ref, hid_ref, nrm_ref,
           heads, w_own, w_other, res_v, send_buf, recv, own, sums,
           local_sem, w_send, w_recv, h_send, h_recv, p_send, p_recv, s_send, s_recv):
    nx = ngy // CORES
    y = lax.axis_index("gx")
    gy = lax.axis_index("gy")
    z = lax.axis_index("gz")
    x, core = lax.div(gy, CORES), lax.rem(gy, CORES)
    in_rows = head_ref.shape[0]
    out_rows, cols = res_ref.shape
    wc = w_ref.shape[1]
    per_block = nz // ny

    def at(dx, dy, dz):
        return (lax.rem(y + dy + ny, ny), lax.rem(x + dx + nx, nx) * CORES + core, lax.rem(z + dz + nz, nz))

    partner = (y, x * CORES + 1 - core, z)
    offsets = {(dx, dy, 0) for dx in range(nx) for dy in range(ny)} | {(dx, 0, dz) for dx in range(nx) for dz in range(nz)}
    offsets = sorted(offsets - {(0, 0, 0)})
    barrier = pltpu.get_barrier_semaphore()
    pl.semaphore_signal(barrier, inc=1, device_id=partner, device_id_type=MESH)
    for off in offsets:
        pl.semaphore_signal(barrier, inc=1, device_id=at(*off), device_id_type=MESH)

    head_in = pltpu.make_async_copy(head_ref, heads.at[0, 0], local_sem.at[0])
    w_in = pltpu.make_async_copy(w_ref, w_own, local_sem.at[1])
    res_in = pltpu.make_async_copy(res_ref, res_v, local_sem.at[2])
    head_in.start()
    w_in.start()
    res_in.start()
    head_in.wait()
    pl.semaphore_wait(barrier, len(offsets) + 1)

    blocks = sorted(((dx, dy) for dx in range(nx) for dy in range(ny)), key=lambda b: ((b[0] > 0) + (b[1] > 0), b))
    head_copies = {}
    for dx, dy in blocks[1:]:
        head_copies[dx, dy] = pltpu.make_async_remote_copy(
            src_ref=heads.at[0, 0], dst_ref=heads.at[dx, dy],
            send_sem=h_send.at[dx, dy], recv_sem=h_recv.at[dx, dy],
            device_id=at(-dx, -dy, 0), device_id_type=MESH)
        head_copies[dx, dy].start()
    w_in.wait()
    w_copy = pltpu.make_async_remote_copy(
        src_ref=w_own, dst_ref=w_other, send_sem=w_send, recv_sem=w_recv,
        device_id=partner, device_id_type=MESH)
    w_copy.start()

    def chunk(dx, dy, hr, j):
        to_z = lax.rem(y + dy, ny) * per_block + j
        dz = lax.rem(to_z - z + nz, nz)
        copy = pltpu.make_async_remote_copy(
            src_ref=send_buf.at[dx, dy, hr, pl.ds(j * out_rows, out_rows)],
            dst_ref=recv.at[dx, dz, hr],
            send_sem=p_send.at[dx, dy, hr, j], recv_sem=p_recv.at[dx, dz, hr],
            device_id=(y, lax.rem(x + dx, nx) * CORES + core, to_z), device_id_type=MESH)
        return to_z, copy

    for dx, dy in blocks:
        if (dx, dy) != (0, 0):
            head_copies[dx, dy].wait_recv()
        for hr in range(CORES):
            if (dx, dy) == (0, 0) and hr == 1:
                w_copy.wait_recv()
            part = jnp.dot(heads[dx, dy], (w_other if hr else w_own)[...], preferred_element_type=F32)
            send_buf[dx, dy, hr] = part.astype(BF16)
            for j in range(per_block):
                to_z, copy = chunk(dx, dy, hr, j)
                if dx:
                    copy.start()
                else:
                    pl.when(to_z != z)(copy.start)

                    @pl.when(to_z == z)
                    def _():
                        own[hr] = part[j * out_rows:(j + 1) * out_rows]

    res_in.wait()
    total = jnp.zeros((out_rows, 128), F32)
    for dx in range(nx):
        from_x = lax.rem(x - dx + nx, nx)
        for hr in range(CORES):
            half = core if hr == 0 else 1 - core
            where = pl.ds(pl.multiple_of((from_x * CORES + half) * wc, wc), wc)
            acc = own[hr] if dx == 0 else None
            for dz in range(nz):
                if (dx, dz) == (0, 0):
                    continue
                pltpu.make_async_remote_copy(
                    src_ref=send_buf.at[0, 0, hr, pl.ds(0, out_rows)], dst_ref=recv.at[dx, dz, hr],
                    send_sem=p_send.at[0, 0, hr, 0], recv_sem=p_recv.at[dx, dz, hr],
                    device_id=partner, device_id_type=MESH).wait_recv()
                term = recv[dx, dz, hr].astype(F32)
                acc = term if acc is None else acc + term
            hidden = (res_v[:, where].astype(F32) + acc).astype(BF16)
            hid_ref[:, where] = hidden
            wide = hidden.astype(F32)
            square = wide * wide
            for k in range(0, wc, 128):
                total = total + square[:, k:k + 128]
    sums[0] = jnp.broadcast_to(jnp.sum(total, axis=1, keepdims=True), (out_rows, 128))
    sum_copies = []
    for dy in range(1, ny):
        sum_copies.append(pltpu.make_async_remote_copy(
            src_ref=sums.at[0], dst_ref=sums.at[dy], send_sem=s_send.at[dy], recv_sem=s_recv.at[dy],
            device_id=at(0, -dy, 0), device_id_type=MESH))
        sum_copies[-1].start()

    w_copy.wait_send()
    for copy in head_copies.values():
        copy.wait_send()
    for dx, dy in blocks:
        for hr in range(CORES):
            for j in range(per_block):
                to_z, copy = chunk(dx, dy, hr, j)
                if dx:
                    copy.wait_send()
                else:
                    pl.when(to_z != z)(copy.wait_send)
    squares = sums[0]
    for dy, copy in enumerate(sum_copies, 1):
        copy.wait()
        squares = squares + sums[dy]
    inverse = lax.rsqrt(squares / (cols * ny) + 1e-05)[:, :1]
    gain = gain_ref[pl.ds(pl.multiple_of(y * cols, cols), cols)].astype(F32).reshape(1, cols)
    nrm_ref[...] = (hid_ref[...].astype(F32) * inverse * gain).astype(BF16)


def shards(head_out, out_weight, residual, norm_gain):
    ny, ngy, nz = (lax.axis_size(a) for a in ("gx", "gy", "gz"))
    nx = ngy // CORES
    in_rows, depth = head_out.shape
    wc = out_weight.shape[1]
    out_rows, cols = residual.shape
    per_block = nz // ny
    any_spec = pl.BlockSpec(memory_space=pl.ANY)
    vmem = pl.BlockSpec(memory_space=pltpu.VMEM)
    dma = pltpu.SemaphoreType.DMA
    return pl.pallas_call(
        functools.partial(kernel, ny, ngy, nz),
        out_shape=[jax.ShapeDtypeStruct((out_rows, cols), BF16)] * 2,
        in_specs=[any_spec, any_spec, any_spec, vmem],
        out_specs=[vmem, vmem],
        scratch_shapes=[
            pltpu.VMEM((nx, ny, in_rows, depth), BF16),
            pltpu.VMEM((depth, wc), BF16),
            pltpu.VMEM((depth, wc), BF16),
            pltpu.VMEM((out_rows, cols), BF16),
            pltpu.VMEM((nx, ny, CORES, in_rows, wc), BF16),
            pltpu.VMEM((nx, nz, CORES, out_rows, wc), BF16),
            pltpu.VMEM((CORES, out_rows, wc), F32),
            pltpu.VMEM((ny, out_rows, 128), F32),
            dma((3,)), dma, dma, dma((nx, ny)), dma((nx, ny)),
            dma((nx, ny, CORES, per_block)), dma((nx, nz, CORES)),
            dma((ny,)), dma((ny,)),
        ],
        compiler_params=pltpu.CompilerParams(collective_id=0, has_side_effects=True),
    )(head_out, out_weight, residual, norm_gain)


def solution(mesh):
    in_specs = (P(("gy", "gx"), "gz"), P("gz", ("gx", "gy")), P(("gy", "gz"), "gx"), P())
    out_specs = (P(("gy", "gz"), "gx"), P(("gy", "gz"), "gx"))
    return jax.shard_map(shards, mesh=mesh, in_specs=in_specs, out_specs=out_specs, check_vma=False)
```

```python
import functools

import jax
import jax.numpy as jnp
from jax import lax
from jax.experimental import pallas as pl
from jax.experimental.pallas import tpu as pltpu
from jax.sharding import PartitionSpec as P

MESH = pl.DeviceIdType.MESH
F32 = jnp.float32
BF16 = jnp.bfloat16
CORES = 2


def kernel(ny, ngy, nz, head_ref, w_ref, res_ref, gain_ref, hid_ref, nrm_ref,
           heads, w_own, w_other, res_v, send_buf, recv, own, sums,
           local_sem, w_send, w_recv, h_send, h_recv, p_send, p_recv, s_send, s_recv):
    nx = ngy // CORES
    y = lax.axis_index("gx")
    gy = lax.axis_index("gy")
    z = lax.axis_index("gz")
    x, core = lax.div(gy, CORES), lax.rem(gy, CORES)
    in_rows = head_ref.shape[0]
    out_rows, cols = res_ref.shape
    wc = w_ref.shape[1]
    per_block = nz // ny

    def at(dx, dy, dz):
        return (lax.rem(y + dy + ny, ny), lax.rem(x + dx + nx, nx) * CORES + core, lax.rem(z + dz + nz, nz))

    partner = (y, x * CORES + 1 - core, z)
    offsets = {(dx, dy, 0) for dx in range(nx) for dy in range(ny)} | {(dx, 0, dz) for dx in range(nx) for dz in range(nz)}
    offsets = sorted(offsets - {(0, 0, 0)})
    barrier = pltpu.get_barrier_semaphore()
    pl.semaphore_signal(barrier, inc=1, device_id=partner, device_id_type=MESH)
    for off in offsets:
        pl.semaphore_signal(barrier, inc=1, device_id=at(*off), device_id_type=MESH)

    head_in = pltpu.make_async_copy(head_ref, heads.at[0, 0], local_sem.at[0])
    w_in = pltpu.make_async_copy(w_ref, w_own, local_sem.at[1])
    res_in = pltpu.make_async_copy(res_ref, res_v, local_sem.at[2])
    head_in.start()
    w_in.start()
    res_in.start()
    head_in.wait()
    pl.semaphore_wait(barrier, len(offsets) + 1)

    blocks = sorted(((dx, dy) for dx in range(nx) for dy in range(ny)), key=lambda b: ((b[0] > 0) + (b[1] > 0), -b[0], b))
    head_copies = {}
    for dx, dy in blocks[1:]:
        head_copies[dx, dy] = pltpu.make_async_remote_copy(
            src_ref=heads.at[0, 0], dst_ref=heads.at[dx, dy],
            send_sem=h_send.at[dx, dy], recv_sem=h_recv.at[dx, dy],
            device_id=at(-dx, -dy, 0), device_id_type=MESH)
        head_copies[dx, dy].start()
    w_in.wait()
    w_copy = pltpu.make_async_remote_copy(
        src_ref=w_own, dst_ref=w_other, send_sem=w_send, recv_sem=w_recv,
        device_id=partner, device_id_type=MESH)
    w_copy.start()

    def chunk(dx, dy, hr, j):
        to_z = lax.rem(y + dy, ny) * per_block + j
        dz = lax.rem(to_z - z + nz, nz)
        copy = pltpu.make_async_remote_copy(
            src_ref=send_buf.at[dx, dy, hr, pl.ds(j * out_rows, out_rows)],
            dst_ref=recv.at[dx, dz, hr],
            send_sem=p_send.at[dx, dy, hr, j], recv_sem=p_recv.at[dx, dz, hr],
            device_id=(y, lax.rem(x + dx, nx) * CORES + core, to_z), device_id_type=MESH)
        return to_z, copy

    for dx, dy in blocks:
        if (dx, dy) != (0, 0):
            head_copies[dx, dy].wait_recv()
        for hr in range(CORES):
            if (dx, dy) == (0, 0) and hr == 1:
                w_copy.wait_recv()
            part = jnp.dot(heads[dx, dy], (w_other if hr else w_own)[...], preferred_element_type=F32)
            send_buf[dx, dy, hr] = part.astype(BF16)
            for j in range(per_block):
                to_z, copy = chunk(dx, dy, hr, j)
                if dx:
                    copy.start()
                else:
                    pl.when(to_z != z)(copy.start)

                    @pl.when(to_z == z)
                    def _():
                        own[hr] = part[j * out_rows:(j + 1) * out_rows]

    res_in.wait()
    total = jnp.zeros((out_rows, 128), F32)
    for dx in range(nx):
        from_x = lax.rem(x - dx + nx, nx)
        for hr in range(CORES):
            half = core if hr == 0 else 1 - core
            where = pl.ds(pl.multiple_of((from_x * CORES + half) * wc, wc), wc)
            acc = own[hr] if dx == 0 else None
            for dz in range(nz):
                if (dx, dz) == (0, 0):
                    continue
                pltpu.make_async_remote_copy(
                    src_ref=send_buf.at[0, 0, hr, pl.ds(0, out_rows)], dst_ref=recv.at[dx, dz, hr],
                    send_sem=p_send.at[0, 0, hr, 0], recv_sem=p_recv.at[dx, dz, hr],
                    device_id=partner, device_id_type=MESH).wait_recv()
                term = recv[dx, dz, hr].astype(F32)
                acc = term if acc is None else acc + term
            hidden = (res_v[:, where].astype(F32) + acc).astype(BF16)
            hid_ref[:, where] = hidden
            wide = hidden.astype(F32)
            square = wide * wide
            for k in range(0, wc, 128):
                total = total + square[:, k:k + 128]
    sums[0] = jnp.broadcast_to(jnp.sum(total, axis=1, keepdims=True), (out_rows, 128))
    sum_copies = []
    for dy in range(1, ny):
        sum_copies.append(pltpu.make_async_remote_copy(
            src_ref=sums.at[0], dst_ref=sums.at[dy], send_sem=s_send.at[dy], recv_sem=s_recv.at[dy],
            device_id=at(0, -dy, 0), device_id_type=MESH))
        sum_copies[-1].start()

    w_copy.wait_send()
    for copy in head_copies.values():
        copy.wait_send()
    for dx, dy in blocks:
        for hr in range(CORES):
            for j in range(per_block):
                to_z, copy = chunk(dx, dy, hr, j)
                if dx:
                    copy.wait_send()
                else:
                    pl.when(to_z != z)(copy.wait_send)
    squares = sums[0]
    for dy, copy in enumerate(sum_copies, 1):
        copy.wait()
        squares = squares + sums[dy]
    inverse = lax.rsqrt(squares / (cols * ny) + 1e-05)[:, :1]
    gain = gain_ref[pl.ds(pl.multiple_of(y * cols, cols), cols)].astype(F32).reshape(1, cols)
    nrm_ref[...] = (hid_ref[...].astype(F32) * inverse * gain).astype(BF16)


def shards(head_out, out_weight, residual, norm_gain):
    ny, ngy, nz = (lax.axis_size(a) for a in ("gx", "gy", "gz"))
    nx = ngy // CORES
    in_rows, depth = head_out.shape
    wc = out_weight.shape[1]
    out_rows, cols = residual.shape
    per_block = nz // ny
    any_spec = pl.BlockSpec(memory_space=pl.ANY)
    vmem = pl.BlockSpec(memory_space=pltpu.VMEM)
    dma = pltpu.SemaphoreType.DMA
    return pl.pallas_call(
        functools.partial(kernel, ny, ngy, nz),
        out_shape=[jax.ShapeDtypeStruct((out_rows, cols), BF16)] * 2,
        in_specs=[any_spec, any_spec, any_spec, vmem],
        out_specs=[vmem, vmem],
        scratch_shapes=[
            pltpu.VMEM((nx, ny, in_rows, depth), BF16),
            pltpu.VMEM((depth, wc), BF16),
            pltpu.VMEM((depth, wc), BF16),
            pltpu.VMEM((out_rows, cols), BF16),
            pltpu.VMEM((nx, ny, CORES, in_rows, wc), BF16),
            pltpu.VMEM((nx, nz, CORES, out_rows, wc), BF16),
            pltpu.VMEM((CORES, out_rows, wc), F32),
            pltpu.VMEM((ny, out_rows, 128), F32),
            dma((3,)), dma, dma, dma((nx, ny)), dma((nx, ny)),
            dma((nx, ny, CORES, per_block)), dma((nx, nz, CORES)),
            dma((ny,)), dma((ny,)),
        ],
        compiler_params=pltpu.CompilerParams(collective_id=0, has_side_effects=True),
    )(head_out, out_weight, residual, norm_gain)


def solution(mesh):
    in_specs = (P(("gy", "gx"), "gz"), P("gz", ("gx", "gy")), P(("gy", "gz"), "gx"), P())
    out_specs = (P(("gy", "gz"), "gx"), P(("gy", "gz"), "gx"))
    return jax.shard_map(shards, mesh=mesh, in_specs=in_specs, out_specs=out_specs, check_vma=False)
```
